32 devices in a mesh: fsdp: 4 (over y, x), tp: 4 (over z), shift: 2 (over core).
Axes of the slice: x: 2, y: 2, z: 4, core: 2. Of those that a mesh axis runs over, the one named last changes fastest.
Arguments:
- w_query: float32 [10240, 5120], P(('shift', 'fsdp'), 'tp'), parts along dimension 0, may hold values from -0.125 to 0.125
- avg_query: float32 [10240, 5120], P(('shift', 'fsdp'), 'tp'), parts along dimension 0, may hold values from -0.078125 to 0.078125
- w_key: float32 [10240, 5120], P(('shift', 'fsdp'), 'tp'), parts along dimension 0, may hold values from -0.125 to 0.125
- avg_key: float32 [10240, 5120], P(('shift', 'fsdp'), 'tp'), parts along dimension 0, may hold values from -0.078125 to 0.078125
- w_value: float32 [10240, 5120], P(('shift', 'fsdp'), 'tp'), parts along dimension 0, may hold values from -0.125 to 0.125
- avg_value: float32 [10240, 5120], P(('shift', 'fsdp'), 'tp'), parts along dimension 0, may hold values from -0.078125 to 0.078125
- norm_train: float32 [10240], P(('shift', 'fsdp', 'tp')), parts along dimension 0, may hold values from 0.25 to 1.75
- norm_step: float32 [10240], P(('shift', 'fsdp', 'tp')), parts along dimension 0, may hold values from -0.3 to 0.3
Outputs:
- ready_query: bfloat16 [10240, 5120], P('shift', 'tp'), parts along dimension 0
- ready_key: bfloat16 [10240, 5120], P('shift', 'tp'), parts along dimension 0
- ready_value: bfloat16 [10240, 5120], P('shift', 'tp'), parts along dimension 0
- scale_query: float32 [10240], P(('shift', 'tp')), parts along dimension 0
- scale_key: float32 [10240], P(('shift', 'tp')), parts along dimension 0
- scale_value: float32 [10240], P(('shift', 'tp')), parts along dimension 0
- serve_norm: bfloat16 [10240], P('shift'), parts along dimension 0
- latest_query: float32 [10240, 5120], P(('shift', 'fsdp'), 'tp'), parts along dimension 0
- latest_key: float32 [10240, 5120], P(('shift', 'fsdp'), 'tp'), parts along dimension 0
- latest_value: float32 [10240, 5120], P(('shift', 'fsdp'), 'tp'), parts along dimension 0
The draws below stay inside these ranges and needn't reach their ends.
There are 2 independent parts, one for each index of `shift`. The reference program is written for one: setup_inputs(seed, part) draws one part's arguments, and reference() takes and returns one part's arrays. A program takes and returns all parts, laid end to end along the dimension named above; each array names one. Nothing has to cross between parts.
All inputs are finite; a program needn't handle non-finite values. Where the reference program divides by a largest or mean magnitude, that divisor is 1e-20 or more.
Results may differ from the reference program's by a relative error of at most 0.001.
Values may be sent and summed in bfloat16 or wider, within the bound.
A program may use at most 192 MiB of HBM per device.

```python
import jax
import jax.numpy as jnp

D_MODEL = 5120
Q_DIM = 5120
KV_DIM = 5120


def raised(drawn, rng, source, target, blocks, factor):
    owner, partner = [(jnp.arange(drawn.shape[dim]) // (drawn.shape[dim] // blocks)).reshape([-1 if axis == dim else 1 for axis in range(drawn.ndim)]) for dim in (source, target)]
    chosen = jax.random.permutation(rng, blocks)[partner]
    strong = (owner == chosen) | (owner == (partner + blocks // 2) % blocks)
    return jnp.where(strong, factor * drawn, drawn)


def steps_of(rng, shape, pieces, low, top_value):
    gain = 1.0
    for dim, blocks in pieces:
        heights = jax.random.uniform(jax.random.fold_in(jax.random.fold_in(rng, 6), dim), (blocks,), jnp.float32, low / len(pieces), top_value / len(pieces))
        gain = gain * jnp.repeat(jnp.exp(heights), shape[dim] // blocks).reshape((-1,) + (1,) * (len(shape) - 1 - dim))
    return gain


def normal_values(own_key, shape, scale, most, cuts=(), dtype=jnp.bfloat16):
    loudness = steps_of(own_key, shape, cuts, -0.22, 0.18) if cuts else 1.0
    entries = jax.random.normal(own_key, shape, jnp.float32) * scale * loudness
    return jnp.minimum(jnp.maximum(entries, -most), most).astype(dtype)


def gaussian_with(stream_key, extent, spread, reach, split, heavy, dtype=jnp.bfloat16):
    values = spread * jax.random.normal(stream_key, extent, jnp.float32)
    if split:
        values = values * steps_of(stream_key, extent, split, -0.22, 0.18)
    return jnp.clip(raised(values, jax.random.fold_in(stream_key, 3), *heavy), -reach, reach).astype(dtype)


def setup_inputs(seed: int = 0, part: int = 0) -> dict:
    splits = jax.random.split(jax.random.key(seed), 9)
    own_keys = jax.random.split(jax.random.fold_in(splits[8], part), 9)
    w_query = gaussian_with(own_keys[0], (D_MODEL, Q_DIM), D_MODEL ** -0.5, 0.125, ((0, 4), (1, 4)), (0, 1, 4, 2.0), jnp.float32)
    avg_query = normal_values(own_keys[1], (D_MODEL, Q_DIM), D_MODEL ** -0.5, 0.078125, ((0, 4), (1, 4)), jnp.float32)
    w_key = gaussian_with(own_keys[2], (D_MODEL, KV_DIM), D_MODEL ** -0.5, 0.125, ((0, 4), (1, 4)), (0, 1, 4, 2.0), jnp.float32)
    avg_key = normal_values(own_keys[3], (D_MODEL, KV_DIM), D_MODEL ** -0.5, 0.078125, ((0, 4), (1, 4)), jnp.float32)
    w_value = gaussian_with(own_keys[4], (D_MODEL, KV_DIM), D_MODEL ** -0.5, 0.125, ((0, 4), (1, 4)), (0, 1, 4, 2.0), jnp.float32)
    avg_value = normal_values(own_keys[5], (D_MODEL, KV_DIM), D_MODEL ** -0.5, 0.078125, ((0, 4), (1, 4)), jnp.float32)
    norm_train = jnp.clip(1.0 + 0.15 * jax.random.normal(own_keys[6], (D_MODEL,), jnp.float32), 0.25, 1.75)
    norm_step = jnp.clip(jax.random.uniform(own_keys[7], (D_MODEL,), jnp.float32, -0.3, 0.3) * steps_of(own_keys[7], (D_MODEL,), ((0, 16),), -0.4, 0.0), -0.3, 0.3)
    return {"w_query": w_query, "avg_query": avg_query, "w_key": w_key, "avg_key": avg_key, "w_value": w_value, "avg_value": avg_value, "norm_train": norm_train, "norm_step": norm_step}


keep_rate = 0.7


def reference(w_query, avg_query, w_key, avg_key, w_value, avg_value, norm_train, norm_step):
    latest_query = keep_rate * avg_query + (1.0 - keep_rate) * w_query
    latest_key = keep_rate * avg_key + (1.0 - keep_rate) * w_key
    latest_value = keep_rate * avg_value + (1.0 - keep_rate) * w_value
    scale_query = jnp.sum(jnp.abs(latest_query), axis=0) / D_MODEL
    ready_query = (latest_query / scale_query).astype(jnp.bfloat16)
    scale_key = jnp.sum(jnp.abs(latest_key), axis=0) / D_MODEL
    ready_key = (latest_key / scale_key).astype(jnp.bfloat16)
    scale_value = jnp.sum(jnp.abs(latest_value), axis=0) / D_MODEL
    ready_value = (latest_value / scale_value).astype(jnp.bfloat16)
    serve_norm = (norm_train + norm_step).astype(jnp.bfloat16)
    return ready_query, ready_key, ready_value, scale_query, scale_key, scale_value, serve_norm, latest_query, latest_key, latest_value
```

```python
import functools

import jax
import jax.numpy as jnp
from jax import lax
from jax.experimental import pallas as pl
from jax.experimental.pallas import tpu as pltpu
from jax.sharding import PartitionSpec as P


keep_rate = 0.7


def place(spots, pieces, base=None, steps=5):
    count = len(pieces)
    rows, cols = pieces[0].shape
    step = rows // steps

    def body(spots_ref, *refs):
        ins, out = refs[:count], refs[-1]
        now = pl.program_id(0)
        for j in range(count):

            @pl.when(now == j)
            def _():
                out[...] = ins[j][...]

    def at(j):
        return lambda g, i, s: (jnp.where(g == j, i, jnp.where(g < j, 0, steps - 1)), 0)

    specs = [pl.BlockSpec((step, cols), at(j)) for j in range(count)]
    operands = list(pieces)
    aliases = {}
    if base is not None:
        specs.append(pl.BlockSpec(memory_space=pl.ANY))
        operands.append(base)
        aliases = {count + 1: 0}
    return pl.pallas_call(
        body,
        grid_spec=pltpu.PrefetchScalarGridSpec(
            num_scalar_prefetch=1,
            grid=(count, steps),
            in_specs=specs,
            out_specs=pl.BlockSpec((step, cols), lambda g, i, s: (s[g] * steps + i, 0)),
        ),
        out_shape=jax.ShapeDtypeStruct((8 * rows, cols), pieces[0].dtype),
        input_output_aliases=aliases,
        cost_estimate=pl.CostEstimate(
            flops=0, bytes_accessed=4 * count * rows * cols, transcendentals=0
        ),
    )(spots, *operands)


def swap(value, axis, bit, size):
    return lax.ppermute(value, axis, [(i, i ^ bit) for i in range(size)])


def gain_of(norm, tp):
    me_t = lax.axis_index("tp")
    parts = [norm] + [
        lax.ppermute(norm, "tp", [(i, (i + s) % tp) for i in range(tp)]) for s in range(1, tp)
    ]
    stacked = jnp.stack(parts)
    order = lax.rem(me_t - jnp.arange(tp) + tp, tp)
    row = jnp.take(stacked, order, axis=0).reshape(-1)
    me = lax.axis_index("fsdp")
    rows = jnp.stack([row] + [swap(row, "fsdp", bit, 4) for bit in (1, 2, 3)])
    return jnp.take(rows, jnp.arange(4) ^ me, axis=0).reshape(-1)


def shards_square(tp, *args):
    norm_train, norm_step = args[6:]
    d_model = 4 * args[0].shape[0]
    me = lax.axis_index("fsdp")
    half = args[0].shape[0] // 2
    latests, scales, readys = [], [], []
    spots = [2 * (me ^ bit) + part for bit in (0, 1, 2) for part in (0, 1)]
    first = jnp.stack(spots).astype(jnp.int32)
    last = jnp.stack([2 * (me ^ 3), 2 * (me ^ 3) + 1]).astype(jnp.int32)
    for w, avg in zip(args[0:6:2], args[1:6:2]):
        latest = keep_rate * avg + (1.0 - keep_rate) * w
        own = jnp.sum(jnp.abs(latest), axis=0)
        by_x, by_y, by_d = (swap(own, "fsdp", bit, 4) for bit in (1, 2, 3))
        scale = ((own + by_x) + (by_y + by_d)) / d_model
        top = (latest[:half] / scale).astype(jnp.bfloat16)
        low = (latest[half:] / scale).astype(jnp.bfloat16)
        x_top = swap(top, "fsdp", 1, 4)
        y_low = swap(low, "fsdp", 2, 4)
        x_low = swap(low, "fsdp", 1, 4)
        y_top = swap(top, "fsdp", 2, 4)
        d_top = swap(x_top, "fsdp", 2, 4)
        d_low = swap(y_low, "fsdp", 1, 4)
        ready = place(first, [top, low, x_top, x_low, y_top, y_low])
        ready = place(last, [d_top, d_low], ready)
        latests.append(latest)
        scales.append(scale)
        readys.append(ready)
    serve_norm = gain_of((norm_train + norm_step).astype(jnp.bfloat16), tp)
    return (*readys, *scales, serve_norm, *latests)


def shards_any(fsdp, *args):
    norm_train, norm_step = args[6:]
    d_model = fsdp * args[0].shape[0]
    latests = [keep_rate * avg + (1.0 - keep_rate) * w for w, avg in zip(args[0:6:2], args[1:6:2])]
    totals = lax.psum(tuple(jnp.sum(jnp.abs(latest), axis=0) for latest in latests), "fsdp")
    scales = [total / d_model for total in totals]
    readys = [
        lax.all_gather((latest / scale).astype(jnp.bfloat16), "fsdp", axis=0, tiled=True)
        for latest, scale in zip(latests, scales)
    ]
    serve_norm = lax.all_gather(
        (norm_train + norm_step).astype(jnp.bfloat16), ("fsdp", "tp"), axis=0, tiled=True
    )
    return (*readys, *scales, serve_norm, *latests)


def solution(mesh):
    weights = P(("shift", "fsdp"), "tp")
    gains = P(("shift", "fsdp", "tp"))
    in_specs = (weights,) * 6 + (gains,) * 2
    out_specs = (P("shift", "tp"),) * 3 + (P(("shift", "tp")),) * 3 + (P("shift"),) + (weights,) * 3
    if mesh.shape["fsdp"] == 4:
        body = functools.partial(shards_square, mesh.shape["tp"])
    else:
        body = functools.partial(shards_any, mesh.shape["fsdp"])
    return jax.shard_map(body, mesh=mesh, in_specs=in_specs, out_specs=out_specs, check_vma=False)
```

```python
import functools

import jax
import jax.numpy as jnp
from jax import lax
from jax.experimental import pallas as pl
from jax.experimental.pallas import tpu as pltpu
from jax.sharding import PartitionSpec as P


keep_rate = 0.7


def place(bits, pieces, base=None, cuts=2):
    count = len(pieces)
    rows, cols = pieces[0].shape
    step = rows // cuts

    def body(*refs):
        ins = refs[:count]
        out, held, read_sem, write_sem = refs[-4:]
        me = lax.axis_index("fsdp")
        reads, writes = [], []
        for j, (bit, part) in enumerate(bits):
            start = (2 * (me ^ bit) + part) * rows
            for c in range(cuts):
                n = j * cuts + c
                spot = pl.ds(pl.multiple_of(start + c * step, step), step)
                reads.append(
                    pltpu.make_async_copy(
                        ins[j].at[pl.ds(c * step, step)], held.at[n], read_sem.at[n]
                    )
                )
                writes.append(pltpu.make_async_copy(held.at[n], out.at[spot], write_sem.at[n]))
        for read in reads:
            read.start()
        for read, write in zip(reads, writes):
            read.wait()
            write.start()
        for write in writes:
            write.wait()

    operands = list(pieces)
    aliases = {}
    if base is not None:
        operands.append(base)
        aliases = {count: 0}
    anywhere = pl.BlockSpec(memory_space=pl.ANY)
    return pl.pallas_call(
        body,
        in_specs=[anywhere] * len(operands),
        out_specs=anywhere,
        out_shape=jax.ShapeDtypeStruct((8 * rows, cols), pieces[0].dtype),
        input_output_aliases=aliases,
        scratch_shapes=[
            pltpu.VMEM((count * cuts, step, cols), pieces[0].dtype),
            pltpu.SemaphoreType.DMA((count * cuts,)),
            pltpu.SemaphoreType.DMA((count * cuts,)),
        ],
        compiler_params=pltpu.CompilerParams(vmem_limit_bytes=16 * 2**20),
        cost_estimate=pl.CostEstimate(
            flops=0, bytes_accessed=4 * count * rows * cols, transcendentals=0
        ),
    )(*operands)


def swap(value, axis, bit, size):
    return lax.ppermute(value, axis, [(i, i ^ bit) for i in range(size)])


def gain_row(norm, tp):
    me_t = lax.axis_index("tp")
    parts = [norm] + [
        lax.ppermute(norm, "tp", [(i, (i + s) % tp) for i in range(tp)]) for s in range(1, tp)
    ]
    order = lax.rem(me_t - jnp.arange(tp) + tp, tp)
    return jnp.take(jnp.stack(parts), order, axis=0).reshape(-1)


def gain_all(row):
    me = lax.axis_index("fsdp")
    rows = jnp.stack([row] + [swap(row, "fsdp", bit, 4) for bit in (1, 2, 3)])
    return jnp.take(rows, jnp.arange(4) ^ me, axis=0).reshape(-1)


tie = lax.optimization_barrier


def blend(w, avg):
    latest = keep_rate * avg + (1.0 - keep_rate) * w
    return latest, jnp.sum(jnp.abs(latest), axis=0)


def total_of(own):
    by_x, by_y, by_d = (swap(own, "fsdp", bit, 4) for bit in (1, 2, 3))
    return (own + by_x) + (by_y + by_d)


def narrow(latest, scale):
    half = latest.shape[0] // 2
    return (
        (latest[:half] / scale).astype(jnp.bfloat16),
        (latest[half:] / scale).astype(jnp.bfloat16),
    )


def spread(top, low):
    x_top = swap(top, "fsdp", 1, 4)
    y_low = swap(low, "fsdp", 2, 4)
    x_low = swap(low, "fsdp", 1, 4)
    y_top = swap(top, "fsdp", 2, 4)
    return x_top, x_low, y_top, y_low


def forward(x_top, y_low):
    return swap(x_top, "fsdp", 2, 4), swap(y_low, "fsdp", 1, 4)


near = [(bit, part) for bit in (0, 1, 2) for part in (0, 1)]
far = [(3, 0), (3, 1)]


def shards_square(tp, w_q, a_q, w_k, a_k, w_v, a_v, norm_train, norm_step):
    d_model = 4 * w_q.shape[0]
    latest_q, own_q = blend(w_q, a_q)
    scale_q = total_of(own_q) / d_model
    top_q, low_q = narrow(latest_q, scale_q)
    w_k, a_k, top_q, low_q = tie((w_k, a_k, top_q, low_q))
    near_q = spread(top_q, low_q)

    latest_k, own_k = blend(w_k, a_k)
    w_v, a_v, own_k = tie((w_v, a_v, own_k))
    latest_v, own_v = blend(w_v, a_v)
    norm_train, norm_step, own_v = tie((norm_train, norm_step, own_v))
    row = gain_row((norm_train + norm_step).astype(jnp.bfloat16), tp)
    row, own_k, own_v = tie((row, own_k, own_v))
    serve_norm = gain_all(row)
    total_k, total_v = total_of(own_k), total_of(own_v)

    far_q = forward(near_q[0], near_q[3])
    serve_norm, total_k, total_v = tie((serve_norm, total_k, total_v))
    scale_k, scale_v = total_k / d_model, total_v / d_model
    top_k, low_k = narrow(latest_k, scale_k)
    near_k = spread(top_k, low_k)
    top_v, low_v = narrow(latest_v, scale_v)
    near_v = spread(top_v, low_v)

    ready_q = place(near, [top_q, low_q, *near_q])
    x_k, y_k, ready_q = tie((near_k[0], near_k[3], ready_q))
    far_k = forward(x_k, y_k)
    ready_q = place(far, far_q, ready_q, 4)
    ready_k = place(near, [top_k, low_k, *near_k])
    x_v, y_v, ready_k, ready_q = tie((near_v[0], near_v[3], ready_k, ready_q))
    far_v = forward(x_v, y_v)
    ready_v = place(near, [top_v, low_v, *near_v])
    ready_v, *far_k = tie((ready_v, *far_k))
    ready_k = place(far, far_k, ready_k, 4)
    ready_k, ready_v = tie((ready_k, ready_v))
    ready_v = place(far, far_v, ready_v, 4)
    return (
        ready_q,
        ready_k,
        ready_v,
        scale_q,
        scale_k,
        scale_v,
        serve_norm,
        latest_q,
        latest_k,
        latest_v,
    )


def shards_any(fsdp, *args):
    norm_train, norm_step = args[6:]
    d_model = fsdp * args[0].shape[0]
    latests = [keep_rate * avg + (1.0 - keep_rate) * w for w, avg in zip(args[0:6:2], args[1:6:2])]
    totals = lax.psum(tuple(jnp.sum(jnp.abs(latest), axis=0) for latest in latests), "fsdp")
    scales = [total / d_model for total in totals]
    readys = [
        lax.all_gather((latest / scale).astype(jnp.bfloat16), "fsdp", axis=0, tiled=True)
        for latest, scale in zip(latests, scales)
    ]
    serve_norm = lax.all_gather(
        (norm_train + norm_step).astype(jnp.bfloat16), ("fsdp", "tp"), axis=0, tiled=True
    )
    return (*readys, *scales, serve_norm, *latests)


def solution(mesh):
    weights = P(("shift", "fsdp"), "tp")
    gains = P(("shift", "fsdp", "tp"))
    in_specs = (weights,) * 6 + (gains,) * 2
    out_specs = (P("shift", "tp"),) * 3 + (P(("shift", "tp")),) * 3 + (P("shift"),) + (weights,) * 3
    if mesh.shape["fsdp"] == 4:
        body = functools.partial(shards_square, mesh.shape["tp"])
    else:
        body = functools.partial(shards_any, mesh.shape["fsdp"])
    return jax.shard_map(body, mesh=mesh, in_specs=in_specs, out_specs=out_specs, check_vma=False)
```
